256 devices in a mesh: dp: 32 (over x, z), col: 8 (over y, core).
Axes of the slice: x: 4, y: 4, z: 8, core: 2. Of those that a mesh axis runs over, the one named last changes fastest.
Arguments:
- activations: bfloat16 [2, 28672, 8192], P(None, 'dp', 'col'), may hold values from -40 to 40
- cotangent: bfloat16 [2, 28672, 2048], P(None, 'dp'), may hold values from -40 to 40
- master_weights: float32 [2, 2048, 8192], P(None, 'dp', 'col'), may hold values from -6 to 6
- moment_codes: bfloat16 [2, 2048, 8192], P(None, 'dp', 'col'), may hold values from -1 to 1
- square_codes: bfloat16 [2, 2048, 8192], P(None, 'dp', 'col'), may hold values from 0.049804688 to 1
- moment_scales: float32 [2, 2048, 4], P(None, 'dp'), may hold values from 0.05 to 0.5
- square_scales: float32 [2, 2048, 4], P(None, 'dp'), may hold values from 0.005 to 0.05
Outputs:
- new_weights: float32 [2, 2048, 8192], P(None, 'dp', 'col')
- new_moment_codes: bfloat16 [2, 2048, 8192], P(None, 'dp', 'col')
- new_square_codes: bfloat16 [2, 2048, 8192], P(None, 'dp', 'col')
- new_moment_scales: float32 [2, 2048, 4], P(None, 'dp')
- new_square_scales: float32 [2, 2048, 4], P(None, 'dp')
The draws below stay inside these ranges and needn't reach their ends.
All inputs are finite; a program needn't handle non-finite values. Where the reference program divides by a largest or mean magnitude, that divisor is 1e-20 or more.
Results may differ from the reference program's by a relative error of at most 0.001.
Values sent between devices are 32-bit elements; how exact they have to be, the bound alone decides.
No kernel may reach another device: no remote copies, remote signals or barrier semaphores. Data moves between devices by JAX's collectives and lax.ppermute only.
A program may use at most 128 MiB of HBM per device.

```python
import math
import jax
import jax.numpy as jnp
from jax import lax

D = 8192
KV = 2048
BLOCK = 2048
LAYERS = 2
STEP = 10
TOK_DEV = 896
TOKENS = 28672
NB = 4
N_DP = 32


def scaled_values(key, width):
    keys = jax.random.split(key, 2)
    position = jnp.arange(width, dtype=jnp.float32) / width
    col_scale = jnp.exp(jnp.log(3.0) * position + jnp.log(3.4) * jax.random.uniform(keys[1], (width,)))
    values = jax.random.normal(keys[0], (LAYERS, TOKENS, width)) * col_scale
    return jnp.clip(values, -40.0, 40.0).astype(jnp.bfloat16)


def draw_activations(key, part):
    return scaled_values(jax.random.fold_in(key, 11), D)


def draw_cotangent(key, part):
    return scaled_values(jax.random.fold_in(key, 23), KV)


def shard_levels(stream_key, shape, cuts, smallest, high):
    def one(axis_at, parts):
        heights = jax.random.uniform(jax.random.fold_in(jax.random.fold_in(stream_key, 6), axis_at), (parts,), jnp.float32, smallest / len(cuts), high / len(cuts))
        return jnp.repeat(jnp.exp(heights), shape[axis_at] // parts).reshape((-1,) + (1,) * (len(shape) - axis_at - 1))

    gain = one(*cuts[0])
    for cut in cuts[1:]:
        gain = gain * one(*cut)
    return gain


def normal_values(stream_key, shape, scale, limit, shards=(), kind=jnp.bfloat16):
    array = scale * jax.random.normal(stream_key, shape, jnp.float32)
    if shards:
        array = array * shard_levels(stream_key, shape, shards, -0.22, 0.18)
    return jnp.clip(array, -limit, limit).astype(kind)


def setup_inputs(seed: int = 0) -> dict:
    arg_keys = jax.random.split(jax.random.key(seed), 8)
    return {
        "activations": draw_activations(jax.random.fold_in(arg_keys[7], 71), 0),
        "cotangent": draw_cotangent(jax.random.fold_in(arg_keys[7], 71), 0),
        "master_weights": normal_values(arg_keys[2], (LAYERS, KV, D), 1.0, 6.0, ((1, 32), (2, 8)), jnp.float32),
        "moment_codes": jnp.clip(jax.random.uniform(arg_keys[3], (LAYERS, KV, D), jnp.float32, -1.0, 1.0) * shard_levels(arg_keys[3], (LAYERS, KV, D), ((1, 32), (2, 8)), -0.4, 0.0), -1.0, 1.0).astype(jnp.bfloat16),
        "square_codes": jnp.clip(0.049804688 + 0.9501953 * jax.random.uniform(arg_keys[4], (LAYERS, KV, D), jnp.float32) ** shard_levels(arg_keys[4], (LAYERS, KV, D), ((1, 32), (2, 8)), -0.2, 0.2), 0.049804688, 1.0).astype(jnp.bfloat16),
        "moment_scales": jnp.clip(jnp.exp(math.log(0.5) - 2.3025851 * jax.random.uniform(arg_keys[5], (LAYERS, KV, NB), jnp.float32) ** shard_levels(arg_keys[5], (LAYERS, KV, NB), ((1, 32),), -0.2, 0.2)), 0.05, 0.5),
        "square_scales": jnp.clip(jnp.exp(math.log(0.05) - 2.3025851 * jax.random.uniform(arg_keys[6], (LAYERS, KV, NB), jnp.float32) ** shard_levels(arg_keys[6], (LAYERS, KV, NB), ((1, 32),), -0.2, 0.2)), 0.005, 0.05),
    }


beta_one = 0.9
beta_two = 0.999
learn_rate = 0.001
decay_rate = 0.1
adam_eps = 1e-08
scale_eps = 1e-06
norm_eps = 1e-06

def layer_gradient(layer_acts, layer_cot):
    grouped_acts = layer_acts.reshape(N_DP, TOK_DEV, D)
    grouped_cot = layer_cot.reshape(N_DP, TOK_DEV, KV)

    def accumulate(total, pair):
        group_acts, group_cot = pair
        partial_sum = lax.dot_general(group_cot, group_acts, (((0,), (0,)), ((), ())), preferred_element_type=jnp.float32)
        return (total + partial_sum, None)
    total, unused = lax.scan(accumulate, jnp.zeros((KV, D), jnp.float32), (grouped_acts, grouped_cot))
    return total

def reference(activations, cotangent, master_weights, moment_codes, square_codes, moment_scales, square_scales):
    gradients = [layer_gradient(activations[index], cotangent[index]) for index in range(LAYERS)]
    total_sq = jnp.float32(0.0)
    for gradient in gradients:
        total_sq = total_sq + jnp.sum(gradient * gradient)
    rms = jnp.sqrt(total_sq / float(LAYERS * KV * D) + norm_eps)
    clip_factor = jnp.minimum(1.0, 1.0 / rms)
    correct_one = 1.0 - beta_one ** STEP
    correct_two = 1.0 - beta_two ** STEP
    outs_weights, outs_mcode, outs_scode, outs_mscale, outs_sscale = ([], [], [], [], [])
    for index in range(LAYERS):
        old_moment = moment_codes[index].astype(jnp.float32).reshape(KV, NB, BLOCK) * moment_scales[index][:, :, None]
        old_square = square_codes[index].astype(jnp.float32).reshape(KV, NB, BLOCK) * square_scales[index][:, :, None]
        grad_now = (clip_factor * gradients[index]).reshape(KV, NB, BLOCK)
        moment = beta_one * old_moment + (1.0 - beta_one) * grad_now
        square = beta_two * old_square + (1.0 - beta_two) * grad_now * grad_now
        moment_max = lax.optimization_barrier(jnp.max(jnp.abs(moment), axis=2))
        square_max = lax.optimization_barrier(jnp.max(square, axis=2))
        outs_mcode.append((moment / (moment_max[:, :, None] + scale_eps)).astype(jnp.bfloat16).reshape(KV, D))
        outs_scode.append((square / (square_max[:, :, None] + scale_eps)).astype(jnp.bfloat16).reshape(KV, D))
        outs_mscale.append(moment_max)
        outs_sscale.append(square_max)
        ratio = (moment / correct_one / (jnp.sqrt(square / correct_two) + adam_eps)).reshape(KV, D)
        weights = master_weights[index]
        outs_weights.append(weights - learn_rate * (decay_rate * weights + ratio))
    return (jnp.stack(outs_weights), jnp.stack(outs_mcode), jnp.stack(outs_scode), jnp.stack(outs_mscale), jnp.stack(outs_sscale))
```

```python
import jax
import jax.numpy as jnp
from jax import lax
from jax.experimental import pallas as pl
from jax.experimental.pallas import tpu as pltpu
from jax.sharding import Mesh
from jax.sharding import PartitionSpec as P

D = 8192
KV = 2048
BLOCK = 2048
LAYERS = 2
STEP = 10
NX = 4
NZ = 8
ROWS = 64
DP = ("x", "z")
COL = ("y", "core")
ALL = ("x", "z", "y", "core")


beta_one = 0.9
beta_two = 0.999
learn_rate = 0.001
decay_rate = 0.1
adam_eps = 1e-08
scale_eps = 1e-06
norm_eps = 1e-06


LANES = 128
WB = 1024
HB = WB // 2
WA = 2048 - WB
COLS = 1024
F32 = jnp.float32


def shifted(array, axis, size, step):
    return lax.ppermute(array, axis, [(i, (i + step) % size) for i in range(size)])


def product(act, cot, layer, rows, col, width):
    lhs = cot[layer, :, pl.ds(pl.multiple_of(rows, LANES), LANES)]
    rhs = act[layer, :, col : col + width]
    return lax.dot_general(lhs, rhs, (((0,), (0,)), ((), ())), preferred_element_type=F32)


def b_rows(ctx, k, half, xb):
    at = lax.rem(ctx.z + k + NZ, NZ)
    both = product(ctx.act, ctx.cot, 1, xb * 512 + at // 2 * LANES, half * HB, HB)
    return jnp.where(lax.rem(at, 2) == 0, both[:ROWS], both[ROWS:])


def a_rows(ctx, k, pair):
    at = lax.rem(ctx.x + k + NX, NX)
    of = lax.rem(ctx.z // 2 + pair + 4, 4)
    rows = at * 512 + of * LANES
    first = product(ctx.act, ctx.cot, 0, rows, 0, COLS)
    if WA == COLS:
        return first
    return jnp.concatenate([first, product(ctx.act, ctx.cot, 1, rows, WB, WA - COLS)], axis=1)


class Job:
    def __init__(self, shape, fill, *inputs):
        self.shape, self.fill, self.inputs = shape, fill, inputs


def b_send(k, half, carried=None):
    def fill(ctx, out, *refs):
        for xb in range(NX):
            value = b_rows(ctx, k, half, xb)
            out[xb] = value + refs[0][xb] if refs else value

    return Job((NX, ROWS, HB), fill, *(() if carried is None else (carried,)))


def a_send(k, pair, carried=None):
    def fill(ctx, out, *refs):
        value = a_rows(ctx, k, pair)
        out[...] = value + refs[0][...] if refs else value

    return Job((2 * ROWS, WA), fill, *(() if carried is None else (carried,)))


def a_done(pairs, arrived):
    def fill(ctx, out, *refs):
        for i, pair in enumerate(pairs):
            value = a_rows(ctx, 0, pair) + refs[2 * i][...] + refs[2 * i + 1][...]
            out[2 * i] = value[:ROWS]
            out[2 * i + 1] = value[ROWS:]

    return Job((4, ROWS, WA), fill, *arrived)


def a_block(ctx, k, low, high):
    odd = lax.rem(ctx.z, 2)
    at = k + 4
    if at + 1 < 4:
        return low[at + odd]
    if 4 <= at and at + 1 < 8:
        return high[at - 4 + odd]
    if at == 3:
        return jnp.where(odd == 0, low[3], high[0])
    return jnp.where(odd == 0, high[3], low[0])


def az_send(k, low, high, carried=None):
    inputs = [a for a in (low, high, carried) if a is not None]

    def fill(ctx, out, *refs):
        refs = list(refs)
        low_ref = refs.pop(0) if low is not None else None
        high_ref = refs.pop(0) if high is not None else None
        value = a_block(ctx, k, low_ref, high_ref)
        out[...] = value + refs[0][...] if refs else value

    return Job((ROWS, WA), fill, *inputs)


def b_done(half, minus, plus):
    def fill(ctx, out, minus_ref, plus_ref):
        for xb in range(NX):
            out[xb] = b_rows(ctx, 0, half, xb) + minus_ref[xb] + plus_ref[xb]

    return Job((NX, ROWS, HB), fill, minus, plus)


def bx_send(k, total, carried=None):
    def fill(ctx, out, *refs):
        refs = list(refs)
        ref = ctx.outs[total] if isinstance(total, int) else refs.pop(0)
        value = ref[lax.rem(ctx.x + k + NX, NX)]
        out[...] = value + refs[0][...] if refs else value

    inputs = [a for a in (total, carried) if a is not None and not isinstance(a, int)]
    return Job((ROWS, HB), fill, *inputs)


class Context:
    pass


def tick(place, act, cot, jobs, after=None, name=None):
    extra = [] if after is None else [after]

    def body(place_ref, act_ref, cot_ref, *refs):
        ctx = Context()
        ctx.x, ctx.z = place_ref[0], place_ref[1]
        ctx.act, ctx.cot = act_ref, cot_ref
        refs = refs[len(extra) :]
        count = sum(len(job.inputs) for job in jobs)
        ins, ctx.outs = refs[:count], refs[count:]
        for job, out in zip(jobs, ctx.outs):
            job.fill(ctx, out, *ins[: len(job.inputs)])
            ins = ins[len(job.inputs) :]

    inputs = [a for job in jobs for a in job.inputs]
    vmem = pl.BlockSpec(memory_space=pltpu.VMEM)
    return pl.pallas_call(
        body,
        out_shape=[jax.ShapeDtypeStruct(job.shape, F32) for job in jobs],
        in_specs=[pl.BlockSpec(memory_space=pltpu.SMEM), vmem, vmem]
        + [pl.BlockSpec(memory_space=pl.ANY)] * len(extra)
        + [vmem] * len(inputs),
        out_specs=[vmem] * len(jobs),
        compiler_params=pltpu.CompilerParams(vmem_limit_bytes=VMEM_LIMIT),
        cost_estimate=pl.CostEstimate(flops=2000000000, bytes_accessed=8000000, transcendentals=0),
        name=name,
    )(place, act, cot, *extra, *inputs)


VMEM_LIMIT = 24 * 1024 * 1024


def summed_gradient(act, cot):
    x, z = lax.axis_index("x"), lax.axis_index("z")
    place = jnp.stack([x, z]).astype(jnp.int32)
    pairs = (-2, -1, 0, 1)
    z_minus = ((4, 0), (3, 1), (3, 0), (2, 1), (2, 0), (1, 1), (1, 0))
    z_plus = ((4, 1), (3, 0), (3, 1), (2, 0), (2, 1), (1, 0), (1, 1))
    x_minus = ((2, 0), (1, 1), (1, 0), (2, 2), (1, 3), (1, 2))
    x_plus = ((2, 1), (1, 0), (1, 1), (2, 3), (1, 2), (1, 3))
    zm, zp, xm, xp = {}, {}, {}, {}
    before = None
    low = am = None
    for t in range(7):
        distance, half = z_minus[t]
        jobs = [b_send(-distance, half, zm.get(half))]
        distance, half = z_plus[t]
        jobs.append(b_send(distance, half, zp.get(half)))
        if t < 6:
            distance, piece = x_minus[t]
            jobs.append(a_send(-distance, pairs[piece], xm.get(piece)))
            distance, piece = x_plus[t]
            jobs.append(a_send(distance, pairs[piece], xp.get(piece)))
        if t == 4:
            jobs.append(a_done(pairs[:2], (xm[0], xp[0], xm[1], xp[1])))
        if t == 6:
            jobs.append(az_send(-3, low, None, am))
        outs = list(tick(place, act, cot, jobs, before, "tick%d" % t))
        before = outs[0]
        if t == 4:
            low = outs[4]
            (start,) = tick(place, act, cot, [az_send(-4, low, None)], None, "far")
            am = shifted(start, "z", NZ, -1)
        if t == 6:
            am = shifted(outs[2], "z", NZ, -1)
        zm[z_minus[t][1]] = shifted(outs[0], "z", NZ, -1)
        zp[z_plus[t][1]] = shifted(outs[1], "z", NZ, 1)
        if t < 6:
            xm[x_minus[t][1]] = shifted(outs[2], "x", NX, -1)
            xp[x_plus[t][1]] = shifted(outs[3], "x", NX, 1)
    (high,) = tick(
        place, act, cot, [a_done(pairs[2:], (xm[2], xp[2], xm[3], xp[3]))], before, "high"
    )
    (start,) = tick(place, act, cot, [az_send(3, low, high)], None, "plus")
    ap = shifted(start, "z", NZ, 1)
    outs = tick(
        place,
        act,
        cot,
        [
            b_done(0, zm[0], zp[0]),
            b_done(1, zm[1], zp[1]),
            bx_send(-2, 0),
            bx_send(1, 0),
            bx_send(2, 1),
            bx_send(-1, 1),
            az_send(-2, low, None, am),
            az_send(2, None, high, ap),
        ],
        None,
        "tick8",
    )
    left, right = outs[:2]
    lm, lp = shifted(outs[2], "x", NX, -1), shifted(outs[3], "x", NX, 1)
    rp, rm = shifted(outs[4], "x", NX, 1), shifted(outs[5], "x", NX, -1)
    am, ap = shifted(outs[6], "z", NZ, -1), shifted(outs[7], "z", NZ, 1)
    outs = tick(
        place,
        act,
        cot,
        [
            bx_send(-1, left, lm),
            bx_send(1, right, rp),
            az_send(-1, low, high, am),
            az_send(1, None, high, ap),
        ],
        None,
        "tick9",
    )
    lm, rp = shifted(outs[0], "x", NX, -1), shifted(outs[1], "x", NX, 1)
    am, ap = shifted(outs[2], "z", NZ, -1), shifted(outs[3], "z", NZ, 1)

    def last(ctx, out, left_ref, lm_ref, lp_ref, right_ref, rm_ref, rp_ref, high_ref, am_ref, ap_ref):
        own_a = a_block(ctx, 0, None, high_ref) + am_ref[...] + ap_ref[...]
        own_l = left_ref[ctx.x] + lm_ref[...] + lp_ref[...]
        own_r = right_ref[ctx.x] + rm_ref[...] + rp_ref[...]
        out[0] = own_a[:, :COLS]
        out[1, :, :HB] = own_l
        out[1, :, HB:WB] = own_r
        if WB < COLS:
            out[1, :, WB:] = own_a[:, COLS:]

    job = Job((2, ROWS, COLS), last, left, lm, lp, right, rm, rp, high, am, ap)
    (gradient,) = tick(place, act, cot, [job], None, "last")
    return gradient


def sent_to_all(array, axis):
    copies = jnp.broadcast_to(array, (lax.axis_size(axis), *array.shape))
    return lax.all_to_all(copies, axis, split_axis=0, concat_axis=0, tiled=True)


def local(
    activations, cotangent, master_weights, moment_codes, square_codes, moment_scales, square_scales
):
    layer_count = activations.shape[0]
    shard_cols = master_weights.shape[2]
    block_count = moment_scales.shape[2]
    gradient = summed_gradient(activations, cotangent)
    local_sq = jnp.sum(gradient * gradient)
    everyone = sent_to_all(jnp.broadcast_to(local_sq, (1, 128)), ALL)
    total_sq = jnp.sum(everyone[:, 0, 0])
    rms = jnp.sqrt(total_sq / float(LAYERS * KV * D) + norm_eps)
    clip_factor = jnp.minimum(1.0, 1.0 / rms)
    correct_one = 1.0 - beta_one**STEP
    correct_two = 1.0 - beta_two**STEP
    own_block = lax.axis_index(COL) * shard_cols // BLOCK
    selector = (jnp.arange(block_count, dtype=jnp.int32) == own_block).astype(jnp.float32)

    def new_moments(layer_index):
        moment_scale = jnp.sum(moment_scales[layer_index] * selector, axis=1)
        square_scale = jnp.sum(square_scales[layer_index] * selector, axis=1)
        old_moment = moment_codes[layer_index].astype(jnp.float32) * moment_scale[:, None]
        old_square = square_codes[layer_index].astype(jnp.float32) * square_scale[:, None]
        grad_now = clip_factor * gradient[layer_index]
        moment = beta_one * old_moment + (1.0 - beta_one) * grad_now
        square = beta_two * old_square + (1.0 - beta_two) * grad_now * grad_now
        return (moment, square, jnp.max(jnp.abs(moment), axis=1), jnp.max(square, axis=1))

    states = [new_moments(layer_index) for layer_index in range(layer_count)]
    own_max = jnp.stack([jnp.stack([s[2] for s in states]), jnp.stack([s[3] for s in states])])
    every_max = sent_to_all(own_max.reshape(1, -1), COL)
    block_max = jnp.max(every_max.reshape(block_count, 2, 2, layer_count, ROWS), axis=1)
    scales = jnp.transpose(block_max, (1, 2, 3, 0))
    moment_maxima, square_maxima = scales[0], scales[1]
    outs_weights, outs_mcode, outs_scode = ([], [], [])
    for layer_index in range(layer_count):
        moment, square = (states[layer_index][0], states[layer_index][1])
        moment_div = jnp.sum(moment_maxima[layer_index] * selector, axis=1)[:, None]
        square_div = jnp.sum(square_maxima[layer_index] * selector, axis=1)[:, None]
        outs_mcode.append((moment / (moment_div + scale_eps)).astype(jnp.bfloat16))
        outs_scode.append((square / (square_div + scale_eps)).astype(jnp.bfloat16))
        ratio = moment / correct_one / (jnp.sqrt(square / correct_two) + adam_eps)
        weights = master_weights[layer_index]
        outs_weights.append(weights - learn_rate * (decay_rate * weights + ratio))
    return (
        jnp.stack(outs_weights),
        jnp.stack(outs_mcode),
        jnp.stack(outs_scode),
        moment_maxima,
        square_maxima,
    )


def solution(mesh):
    split = Mesh(mesh.devices.reshape(NX, NZ, 4, 2), ALL)
    in_specs = (
        P(None, DP, COL),
        P(None, DP, None),
        P(None, DP, COL),
        P(None, DP, COL),
        P(None, DP, COL),
        P(None, DP, None),
        P(None, DP, None),
    )
    out_specs = (
        P(None, DP, COL),
        P(None, DP, COL),
        P(None, DP, COL),
        P(None, DP, None),
        P(None, DP, None),
    )
    return jax.shard_map(local, mesh=split, in_specs=in_specs, out_specs=out_specs, check_vma=False)
```
